32 devices in a mesh: ens: 2 (over x), time: 4 (over z), chan: 4 (over y, core).
Axes of the slice: x: 2, y: 2, z: 4, core: 2. Of those that a mesh axis runs over, the one named last changes fastest.
Arguments:
- decay_rate: float32 [4, 4096, 1024], P('ens', 'time', 'chan'), parts along dimension 0, may hold values from 0.2 to 2
- drive_in: bfloat16 [4, 4096, 1024], P('ens', 'time', 'chan'), parts along dimension 0, may hold values from -6 to 6
- gate_in: bfloat16 [4, 4096, 1024], P('ens', 'time', 'chan'), parts along dimension 0, may hold values from -6 to 6
- norm_gain: float32 [2048], P(('ens', 'chan')), parts along dimension 0, may hold values from 0.25 to 1.75
Outputs:
- mixed_out: bfloat16 [4, 4096, 1024], P('ens', 'time', 'chan'), parts along dimension 0
The draws below stay inside these ranges and needn't reach their ends.
There are 2 independent parts, one for each index of `ens`. The reference program is written for one: setup_inputs(seed, part) draws one part's arguments, and reference() takes and returns one part's arrays. A program takes and returns all parts, laid end to end along the dimension named above; each array names one. Nothing has to cross between parts.
All inputs are finite; a program needn't handle non-finite values.
Results may differ from the reference program's by a relative error of at most 0.001.
Values sent between devices are 32-bit elements.
A program may use at most 64 MiB of HBM per device.

```python
import jax
import jax.numpy as jnp
from jax import lax

BATCH = 2
CHANNELS = 1024
LENGTH = 4096


def steps_of(stream_key, shape, pieces, least, high):
    level = 1.0
    for dim, parts in pieces:
        steps = jax.random.uniform(jax.random.fold_in(jax.random.fold_in(stream_key, 6), dim), (parts,), jnp.float32, least / len(pieces), high / len(pieces))
        level = level * jnp.repeat(jnp.exp(steps), shape[dim] // parts).reshape((-1,) + (1,) * (len(shape) - 1 - dim))
    return level


def scatter_about(key, dims, width, limit, shards=(), held_as=jnp.bfloat16):
    entries = width * jax.random.normal(key, dims, jnp.float32)
    if shards:
        entries = entries * steps_of(key, dims, shards, -0.22, 0.18)
    return jnp.clip(entries, -limit, limit).astype(held_as)


def setup_inputs(seed: int = 0, part: int = 0) -> dict:
    seeds = jax.random.split(jax.random.key(seed), 5)
    part_keys = jax.random.split(jax.random.fold_in(seeds[4], part), 5)
    return {
        "decay_rate": jnp.clip(0.2 + 1.8 * jax.random.uniform(part_keys[0], (BATCH, LENGTH, CHANNELS), jnp.float32) ** steps_of(part_keys[0], (BATCH, LENGTH, CHANNELS), ((1, 4), (2, 4)), -0.2, 0.2), 0.2, 2.0),
        "drive_in": scatter_about(part_keys[1], (BATCH, LENGTH, CHANNELS), 1.0, 6.0, ((1, 4), (2, 4))),
        "gate_in": scatter_about(part_keys[2], (BATCH, LENGTH, CHANNELS), 1.0, 6.0, ((1, 4), (2, 4))),
        "norm_gain": jnp.clip(1.0 + 0.15 * jax.random.normal(part_keys[3], (CHANNELS,), jnp.float32), 0.25, 1.75),
    }


def join_pair(earlier, later):
    return (earlier[0] * later[0], later[0] * earlier[1] + later[1])

def reference(decay_rate, drive_in, gate_in, norm_gain):
    keep = jnp.exp(-decay_rate / LENGTH)
    push = drive_in.astype(jnp.float32) * LENGTH ** (-0.5)
    forward = lax.associative_scan(join_pair, (keep, push), axis=1)[1]
    backward = lax.associative_scan(join_pair, (keep, push), axis=1, reverse=True)[1]
    states = forward + backward
    gated = states * jax.nn.silu(gate_in.astype(jnp.float32))
    power = lax.optimization_barrier(jnp.mean(gated * gated, axis=-1, keepdims=True))
    mixed_out = (gated * lax.rsqrt(power + 1e-06) * norm_gain).astype(jnp.bfloat16)
    return mixed_out
```

```python
import functools

import jax
import jax.numpy as jnp
from jax import lax
from jax.experimental import pallas as pl
from jax.experimental.pallas import tpu as pltpu
from jax.sharding import PartitionSpec as P

MESH = pl.DeviceIdType.MESH
LANES = 128


def split(value):
    high = value.astype(jnp.bfloat16)
    return high, (value - high.astype(jnp.float32)).astype(jnp.bfloat16)


def sums(triangle, value):
    high, low = split(value)
    return jnp.dot(triangle, high, preferred_element_type=jnp.float32) + jnp.dot(
        triangle, low, preferred_element_type=jnp.float32
    )


def kernel(
    batch, span, times, chans, length,
    decay_hbm, drive_hbm, gate_hbm, gain_ref, out_ref,
    base, drive, gate, fall, rise, back,
    stats, entering, mine, others, column, power, powers,
    load_sem, send_sem, recv_sem, power_send_sem, power_recv_sem,
):
    chunks, size, channels = base.shape
    time, chan = lax.axis_index("time"), lax.axis_index("chan")

    def load(which, c):
        source, target = ((decay_hbm, base), (drive_hbm, drive), (gate_hbm, gate))[which]
        return pltpu.make_async_copy(source.at[c], target.at[c], load_sem.at[which, c])

    for c in range(chunks):
        load(0, c).start()
        load(1, c).start()
    for c in range(chunks):
        load(2, c).start()

    barrier = pltpu.get_barrier_semaphore()
    for d in range(1, times):
        pl.semaphore_signal(barrier, inc=1, device_id={"time": lax.rem(time + d, times)}, device_id_type=MESH)
    for d in range(1, chans):
        pl.semaphore_signal(barrier, inc=1, device_id={"chan": lax.rem(chan + d, chans)}, device_id_type=MESH)

    row = lax.broadcasted_iota(jnp.int32, (size, size), 0)
    col = lax.broadcasted_iota(jnp.int32, (size, size), 1)
    lower = jnp.where(row >= col, 1.0, 0.0).astype(jnp.bfloat16)
    upper = jnp.where(row <= col, 1.0, 0.0).astype(jnp.bfloat16)

    def scan(c, _):
        load(0, c).wait()
        load(1, c).wait()
        rate = base[c] * (1.0 / length)
        total = sums(lower, rate)
        push = drive[c].astype(jnp.float32) * length ** (-0.5)
        up, down = jnp.exp(total), jnp.exp(-total)
        fall[c] = down
        rise[c] = up * jnp.exp(-rate)
        ahead = sums(lower, up * push)
        behind = sums(upper, down * jnp.exp(rate) * push)
        base[c] = ahead
        back[c] = behind
        stats[c, 0:1] = down[size - 1 :]
        stats[c, 1:2] = down[size - 1 :] * ahead[size - 1 :]
        stats[c, 2:3] = behind[0:1]
        return _

    lax.fori_loop(0, chunks, scan, 0)

    mine[...] = jnp.zeros(mine.shape, jnp.float32)
    for b in range(batch):
        product = jnp.ones((1, channels), jnp.float32)
        forward = jnp.zeros((1, channels), jnp.float32)
        backward = jnp.zeros((1, channels), jnp.float32)
        for j in range(span):
            keep = stats[b * span + j, 0:1]
            product = product * keep
            forward = keep * forward + stats[b * span + j, 1:2]
        for j in reversed(range(span)):
            backward = stats[b * span + j, 0:1] * backward + stats[b * span + j, 2:3]
        mine[3 * b : 3 * b + 1] = product
        mine[3 * b + 1 : 3 * b + 2] = forward
        mine[3 * b + 2 : 3 * b + 3] = backward

    pl.semaphore_wait(barrier, times + chans - 2)

    def exchange(d):
        return pltpu.make_async_remote_copy(
            src_ref=mine, dst_ref=others.at[d - 1],
            send_sem=send_sem.at[d - 1], recv_sem=recv_sem.at[d - 1],
            device_id={"time": lax.rem(time + d, times)}, device_id_type=MESH,
        )

    for d in range(1, times):
        exchange(d).start()

    def weigh(c, _):
        load(2, c).wait()
        value = gate[c].astype(jnp.float32)
        gated = 0.5 * value * (1.0 + jnp.tanh(0.5 * value))
        ahead, behind = fall[c] * gated, rise[c] * gated
        base[c] = ahead * base[c] + behind * back[c]
        fall[c] = ahead
        rise[c] = behind
        return _

    lax.fori_loop(0, chunks, weigh, 0)

    for d in range(1, times):
        exchange(d).wait()

    for b in range(batch):
        forward = jnp.zeros((1, channels), jnp.float32)
        backward = jnp.zeros((1, channels), jnp.float32)
        for d in reversed(range(1, times)):
            new = others[d - 1, 3 * b : 3 * b + 1] * forward + others[d - 1, 3 * b + 1 : 3 * b + 2]
            forward = jnp.where(time >= d, new, forward)
            slot = times - d - 1
            new = others[slot, 3 * b : 3 * b + 1] * backward + others[slot, 3 * b + 2 : 3 * b + 3]
            backward = jnp.where(time + d < times, new, backward)
        for j in range(span):
            entering[b * span + j, 0:1] = forward
            forward = stats[b * span + j, 0:1] * forward + stats[b * span + j, 1:2]
        for j in reversed(range(span)):
            backward = stats[b * span + j, 0:1] * backward
            entering[b * span + j, 1:2] = backward
            backward = backward + stats[b * span + j, 2:3]

    lane = lax.broadcasted_iota(jnp.int32, (size, LANES), 1)
    column[...] = jnp.zeros((size, LANES), jnp.float32)

    def join(c, _):
        gated = base[c] + fall[c] * entering[c, 0:1] + rise[c] * entering[c, 1:2]
        base[c] = gated
        squares = jnp.sum(gated * gated, axis=-1, keepdims=True)
        column[...] = jnp.where(lane == c, squares, column[...])
        return _

    lax.fori_loop(0, chunks, join, 0)
    power[...] = jnp.transpose(column[...])[: power.shape[0]]

    def spread(d):
        return pltpu.make_async_remote_copy(
            src_ref=power, dst_ref=powers.at[d - 1],
            send_sem=power_send_sem.at[d - 1], recv_sem=power_recv_sem.at[d - 1],
            device_id={"chan": lax.rem(chan + d, chans)}, device_id_type=MESH,
        )

    for d in range(1, chans):
        spread(d).start()
    for d in range(1, chans):
        spread(d).wait()
    total = power[...]
    for d in range(1, chans):
        total = total + powers[d - 1]
    scale = lax.rsqrt(total / (channels * chans) + 1e-06)
    scale = jnp.concatenate([scale, jnp.zeros((LANES - scale.shape[0], size), jnp.float32)], axis=0)
    column[...] = jnp.transpose(scale)
    gain = gain_ref[...]
    for c in range(chunks):
        out_ref[c] = (base[c] * column[:, c : c + 1] * gain).astype(jnp.bfloat16)


def solution(mesh):
    times, chans = mesh.shape["time"], mesh.shape["chan"]

    def local(decay_rate, drive_in, gate_in, norm_gain):
        batch, positions, channels = decay_rate.shape
        size = min(256, positions)
        span = positions // size
        chunks = batch * span
        rows = -(-3 * batch // 8) * 8
        power_rows = -(-chunks // 8) * 8
        whole = (chunks, size, channels)
        out = pl.pallas_call(
            functools.partial(kernel, batch, span, times, chans, positions * times),
            out_shape=pltpu.VMEM(whole, jnp.bfloat16),
            in_specs=[pl.BlockSpec(memory_space=pl.ANY)] * 3 + [pl.BlockSpec(memory_space=pltpu.VMEM)],
            out_specs=pl.BlockSpec(memory_space=pltpu.VMEM),
            scratch_shapes=[
                pltpu.VMEM(whole, jnp.float32),
                pltpu.VMEM(whole, jnp.bfloat16),
                pltpu.VMEM(whole, jnp.bfloat16),
                pltpu.VMEM(whole, jnp.float32),
                pltpu.VMEM(whole, jnp.float32),
                pltpu.VMEM(whole, jnp.float32),
                pltpu.VMEM((chunks, 8, channels), jnp.float32),
                pltpu.VMEM((chunks, 8, channels), jnp.float32),
                pltpu.VMEM((rows, channels), jnp.float32),
                pltpu.VMEM((times - 1, rows, channels), jnp.float32),
                pltpu.VMEM((size, LANES), jnp.float32),
                pltpu.VMEM((power_rows, size), jnp.float32),
                pltpu.VMEM((chans - 1, power_rows, size), jnp.float32),
                pltpu.SemaphoreType.DMA((3, chunks)),
                pltpu.SemaphoreType.DMA((times - 1,)),
                pltpu.SemaphoreType.DMA((times - 1,)),
                pltpu.SemaphoreType.DMA((chans - 1,)),
                pltpu.SemaphoreType.DMA((chans - 1,)),
            ],
            compiler_params=pltpu.CompilerParams(
                collective_id=0, has_side_effects=True, vmem_limit_bytes=60 * 1024 * 1024
            ),
        )(
            decay_rate.reshape(whole),
            drive_in.reshape(whole),
            gate_in.reshape(whole),
            norm_gain.reshape(1, channels),
        )
        return out.reshape(decay_rate.shape)

    in_specs = (
        P("ens", "time", "chan"),
        P("ens", "time", "chan"),
        P("ens", "time", "chan"),
        P(("ens", "chan")),
    )
    return jax.shard_map(
        local, mesh=mesh, in_specs=in_specs, out_specs=P("ens", "time", "chan"), check_vma=False
    )
```

```python
import functools
import math

import jax
import jax.numpy as jnp
from jax import lax
from jax.experimental import pallas as pl
from jax.experimental.pallas import tpu as pltpu
from jax.sharding import PartitionSpec as P

MESH = pl.DeviceIdType.MESH
LANES = 128
GROUP = 4


def steps(chunks, body):
    group = GROUP if chunks % GROUP == 0 else 1

    def step(i, carry):
        for k in range(group):
            body(i * group + k)
        return carry

    lax.fori_loop(0, chunks // group, step, 0)


def split(value):
    high = value.astype(jnp.bfloat16)
    return high, (value - high.astype(jnp.float32)).astype(jnp.bfloat16)


def sums(triangle, value):
    high, low = split(value)
    return jnp.dot(triangle, high, preferred_element_type=jnp.float32) + jnp.dot(
        triangle, low, preferred_element_type=jnp.float32
    )


def kernel(
    batch, span, times, chans, length,
    decay_hbm, drive_hbm, gate_hbm, gain_ref, out_ref,
    base, drive, gate, fall, rise, back,
    stats, entering, mine, others, column, power, powers,
    load_sem, send_sem, recv_sem, power_send_sem, power_recv_sem,
):
    chunks, size, channels = base.shape
    time, chan = lax.axis_index("time"), lax.axis_index("chan")

    def load(which, c):
        source, target = ((decay_hbm, base), (drive_hbm, drive), (gate_hbm, gate))[which]
        return pltpu.make_async_copy(source.at[c], target.at[c], load_sem.at[which, c])

    for c in range(chunks):
        load(0, c).start()
        load(1, c).start()
    for c in range(chunks):
        load(2, c).start()

    barrier = pltpu.get_barrier_semaphore()
    for d in range(1, times):
        pl.semaphore_signal(barrier, inc=1, device_id={"time": lax.rem(time + d, times)}, device_id_type=MESH)
    for d in range(1, chans):
        pl.semaphore_signal(barrier, inc=1, device_id={"chan": lax.rem(chan + d, chans)}, device_id_type=MESH)

    row = lax.broadcasted_iota(jnp.int32, (size, size), 0)
    col = lax.broadcasted_iota(jnp.int32, (size, size), 1)
    lower = jnp.where(row >= col, 1.0, 0.0).astype(jnp.bfloat16)
    upper = jnp.where(row <= col, 1.0, 0.0).astype(jnp.bfloat16)

    def scan(c):
        load(0, c).wait()
        load(1, c).wait()
        rate = base[c] * (math.log2(math.e) / length)
        total = sums(lower, rate)
        push = drive[c].astype(jnp.float32) * length ** (-0.5)
        before = total - rate
        down = jnp.exp2(-total)
        fall[c] = down
        rise[c] = jnp.exp2(before)
        ahead = sums(lower, jnp.exp2(total) * push)
        behind = sums(upper, jnp.exp2(-before) * push)
        base[c] = ahead
        back[c] = behind
        stats[c, 0:1] = down[size - 1 :]
        stats[c, 1:2] = down[size - 1 :] * ahead[size - 1 :]
        stats[c, 2:3] = behind[0:1]

    steps(chunks, scan)

    mine[...] = jnp.zeros(mine.shape, jnp.float32)
    for b in range(batch):
        product = jnp.ones((1, channels), jnp.float32)
        forward = jnp.zeros((1, channels), jnp.float32)
        backward = jnp.zeros((1, channels), jnp.float32)
        for j in range(span):
            keep = stats[b * span + j, 0:1]
            product = product * keep
            forward = keep * forward + stats[b * span + j, 1:2]
        for j in reversed(range(span)):
            backward = stats[b * span + j, 0:1] * backward + stats[b * span + j, 2:3]
        mine[3 * b : 3 * b + 1] = product
        mine[3 * b + 1 : 3 * b + 2] = forward
        mine[3 * b + 2 : 3 * b + 3] = backward

    pl.semaphore_wait(barrier, times + chans - 2)

    def exchange(d):
        return pltpu.make_async_remote_copy(
            src_ref=mine, dst_ref=others.at[d - 1],
            send_sem=send_sem.at[d - 1], recv_sem=recv_sem.at[d - 1],
            device_id={"time": lax.rem(time + d, times)}, device_id_type=MESH,
        )

    for d in range(1, times):
        exchange(d).start()

    def weigh(c):
        load(2, c).wait()
        value = gate[c].astype(jnp.float32)
        gated = 0.5 * value * (1.0 + jnp.tanh(0.5 * value))
        ahead, behind = fall[c] * gated, rise[c] * gated
        base[c] = ahead * base[c] + behind * back[c]
        fall[c] = ahead
        rise[c] = behind

    steps(chunks, weigh)

    for d in range(1, times):
        exchange(d).wait()

    for b in range(batch):
        forward = jnp.zeros((1, channels), jnp.float32)
        backward = jnp.zeros((1, channels), jnp.float32)
        for d in reversed(range(1, times)):
            new = others[d - 1, 3 * b : 3 * b + 1] * forward + others[d - 1, 3 * b + 1 : 3 * b + 2]
            forward = jnp.where(time >= d, new, forward)
            slot = times - d - 1
            new = others[slot, 3 * b : 3 * b + 1] * backward + others[slot, 3 * b + 2 : 3 * b + 3]
            backward = jnp.where(time + d < times, new, backward)
        for j in range(span):
            entering[b * span + j, 0:1] = forward
            forward = stats[b * span + j, 0:1] * forward + stats[b * span + j, 1:2]
        for j in reversed(range(span)):
            backward = stats[b * span + j, 0:1] * backward
            entering[b * span + j, 1:2] = backward
            backward = backward + stats[b * span + j, 2:3]

    lane = lax.broadcasted_iota(jnp.int32, (size, LANES), 1)
    column[...] = jnp.zeros((size, LANES), jnp.float32)

    def join(c):
        gated = base[c] + fall[c] * entering[c, 0:1] + rise[c] * entering[c, 1:2]
        base[c] = gated
        squares = jnp.sum(gated * gated, axis=-1, keepdims=True)
        column[...] = jnp.where(lane == c, squares, column[...])

    steps(chunks, join)
    power[...] = jnp.transpose(column[...])[: power.shape[0]]

    def spread(d):
        return pltpu.make_async_remote_copy(
            src_ref=power, dst_ref=powers.at[d - 1],
            send_sem=power_send_sem.at[d - 1], recv_sem=power_recv_sem.at[d - 1],
            device_id={"chan": lax.rem(chan + d, chans)}, device_id_type=MESH,
        )

    for d in range(1, chans):
        spread(d).start()
    for d in range(1, chans):
        spread(d).wait()
    total = power[...]
    for d in range(1, chans):
        total = total + powers[d - 1]
    scale = lax.rsqrt(total / (channels * chans) + 1e-06)
    scale = jnp.concatenate([scale, jnp.zeros((LANES - scale.shape[0], size), jnp.float32)], axis=0)
    column[...] = jnp.transpose(scale)
    gain = gain_ref[...]
    for c in range(chunks):
        out_ref[c] = (base[c] * column[:, c : c + 1] * gain).astype(jnp.bfloat16)


def solution(mesh):
    times, chans = mesh.shape["time"], mesh.shape["chan"]

    def local(decay_rate, drive_in, gate_in, norm_gain):
        batch, positions, channels = decay_rate.shape
        size = min(256, positions)
        span = positions // size
        chunks = batch * span
        rows = -(-3 * batch // 8) * 8
        power_rows = -(-chunks // 8) * 8
        whole = (chunks, size, channels)
        out = pl.pallas_call(
            functools.partial(kernel, batch, span, times, chans, positions * times),
            out_shape=pltpu.VMEM(whole, jnp.bfloat16),
            in_specs=[pl.BlockSpec(memory_space=pl.ANY)] * 3 + [pl.BlockSpec(memory_space=pltpu.VMEM)],
            out_specs=pl.BlockSpec(memory_space=pltpu.VMEM),
            scratch_shapes=[
                pltpu.VMEM(whole, jnp.float32),
                pltpu.VMEM(whole, jnp.bfloat16),
                pltpu.VMEM(whole, jnp.bfloat16),
                pltpu.VMEM(whole, jnp.float32),
                pltpu.VMEM(whole, jnp.float32),
                pltpu.VMEM(whole, jnp.float32),
                pltpu.VMEM((chunks, 8, channels), jnp.float32),
                pltpu.VMEM((chunks, 8, channels), jnp.float32),
                pltpu.VMEM((rows, channels), jnp.float32),
                pltpu.VMEM((times - 1, rows, channels), jnp.float32),
                pltpu.VMEM((size, LANES), jnp.float32),
                pltpu.VMEM((power_rows, size), jnp.float32),
                pltpu.VMEM((chans - 1, power_rows, size), jnp.float32),
                pltpu.SemaphoreType.DMA((3, chunks)),
                pltpu.SemaphoreType.DMA((times - 1,)),
                pltpu.SemaphoreType.DMA((times - 1,)),
                pltpu.SemaphoreType.DMA((chans - 1,)),
                pltpu.SemaphoreType.DMA((chans - 1,)),
            ],
            compiler_params=pltpu.CompilerParams(
                collective_id=0, has_side_effects=True, vmem_limit_bytes=60 * 1024 * 1024
            ),
        )(
            decay_rate.reshape(whole),
            drive_in.reshape(whole),
            gate_in.reshape(whole),
            norm_gain.reshape(1, channels),
        )
        return out.reshape(decay_rate.shape)

    in_specs = (
        P("ens", "time", "chan"),
        P("ens", "time", "chan"),
        P("ens", "time", "chan"),
        P(("ens", "chan")),
    )
    return jax.shard_map(
        local, mesh=mesh, in_specs=in_specs, out_specs=P("ens", "time", "chan"), check_vma=False
    )
```
